32 devices in a mesh: part: 1 (over z), tpa: 4 (over y), tpb: 8 (over x, core).
Axes of the slice: x: 4, y: 4, z: 1, core: 2. Of those that a mesh axis runs over, the one named last changes fastest.
The devices are a block of a 4x4x8 slice.
Arguments:
- x: bfloat16 [8, 1024, 4096], P(('part', 'tpb'))
- lengths: int32 [8], P(('part', 'tpb'))
- k_buf: bfloat16 [8, 1024, 32, 128], P(('part', 'tpb'), None, 'tpa')
- v_buf: bfloat16 [8, 1024, 32, 128], P(('part', 'tpb'), None, 'tpa')
- w_qkv: bfloat16 [4096, 12288], P('part', ('tpa', 'tpb'))
- w_o: bfloat16 [4096, 4096], P(('part', 'tpa', 'tpb'))
- w_gate_up: bfloat16 [4096, 22016], P('part', ('tpa', 'tpb'))
- w_down: bfloat16 [11008, 4096], P(('part', 'tpa', 'tpb'))
- g_attn: bfloat16 [4096], P('part')
- g_mlp: bfloat16 [4096], P('part')
Outputs:
- output 1: bfloat16 [8, 1024, 4096], P(('part', 'tpb'))
- output 2: bfloat16 [8, 1024, 32, 128], P(('part', 'tpb'), None, 'tpa')
- output 3: bfloat16 [8, 1024, 32, 128], P(('part', 'tpb'), None, 'tpa')
- output 4: bfloat16 [4096, 4096], P('part', 'tpa')
- output 5: bfloat16 [4096, 4096], P('part', 'tpa')
- output 6: bfloat16 [4096, 4096], P('part', 'tpa')
- output 7: bfloat16 [4096, 4096], P(('part', 'tpa'))
- output 8: bfloat16 [4096, 11008], P('part', 'tpa')
- output 9: bfloat16 [4096, 11008], P('part', 'tpa')
- output 10: bfloat16 [11008, 4096], P(('part', 'tpa'))
All inputs are finite; a program needn't handle non-finite values.
Results may differ from the reference program's by a relative error of at most 0.0139058.
Values are sent between devices in bfloat16 or wider.
A program may use at most 768 MiB of HBM per device.

```python
import math
import jax
import jax.numpy as jnp
from jax import lax

D = 4096
HEADS = 32
KV_HEADS = 32
HEAD = 128
FF = 11008
BATCH = 8
SEQ = 1024
TRAIN_TP = 32
GROUP = HEADS // KV_HEADS
QKV_COLS = KV_HEADS * (GROUP + 2) * HEAD
FF_BLOCK = FF // TRAIN_TP
ROPE_BASE = 500000.0
ROPE_FACTOR = 8.0
LOW_FREQ = 1.0
HIGH_FREQ = 4.0
ORIG_CONTEXT = 8192.0
NORM_EPS = 1e-5
MASK_VALUE = -1e30


def setup_inputs(seed: int = 0, part: int = 0) -> dict:
    part_key = jax.random.fold_in(jax.random.key(seed), part)
    sub_keys = jax.random.split(part_key, 10)
    x_in = jax.random.normal(sub_keys[0], (BATCH, SEQ, D), jnp.float32)
    drawn_len = jax.random.randint(sub_keys[1], (BATCH,), 1, SEQ + 1)
    lengths = jnp.where(jnp.arange(BATCH) == 0, SEQ, drawn_len).astype(jnp.int32)
    k_buf = jax.random.normal(sub_keys[2], (BATCH, SEQ, KV_HEADS, HEAD), jnp.float32)
    v_buf = jax.random.normal(sub_keys[3], (BATCH, SEQ, KV_HEADS, HEAD), jnp.float32)
    qk_scale = jnp.where(jnp.arange(GROUP + 2) <= GROUP, 1.5, 1.0)[:, None]
    w_qkv = (jax.random.normal(sub_keys[4], (D, KV_HEADS, GROUP + 2, HEAD), jnp.float32) * qk_scale * D ** -0.5).reshape(D, QKV_COLS)
    w_o = jax.random.normal(sub_keys[5], (HEADS * HEAD, D), jnp.float32) * (HEADS * HEAD) ** -0.5
    w_gate_up = jax.random.normal(sub_keys[6], (D, 2 * FF), jnp.float32) * D ** -0.5
    w_down = jax.random.normal(sub_keys[7], (FF, D), jnp.float32) * FF ** -0.5
    g_attn = 1.0 + 0.4 * jax.random.normal(sub_keys[8], (D,), jnp.float32)
    g_mlp = 1.0 + 0.4 * jax.random.normal(sub_keys[9], (D,), jnp.float32)
    return {'x': x_in.astype(jnp.bfloat16), 'lengths': lengths, 'k_buf': k_buf.astype(jnp.bfloat16), 'v_buf': v_buf.astype(jnp.bfloat16), 'w_qkv': w_qkv.astype(jnp.bfloat16), 'w_o': w_o.astype(jnp.bfloat16), 'w_gate_up': w_gate_up.astype(jnp.bfloat16), 'w_down': w_down.astype(jnp.bfloat16), 'g_attn': g_attn.astype(jnp.bfloat16), 'g_mlp': g_mlp.astype(jnp.bfloat16)}


def rms_norm(x_in, gain_vec):
    x_wide = x_in.astype(jnp.float32)
    mean_sq = jnp.mean(x_wide * x_wide, axis=-1, keepdims=True)
    return (x_wide * lax.rsqrt(mean_sq + NORM_EPS) * gain_vec.astype(jnp.float32)).astype(jnp.bfloat16)


def rope_tables():
    exponent = jnp.arange(HEAD // 2, dtype=jnp.float32) * (2.0 / HEAD)
    inv_freq = 1.0 / jnp.power(ROPE_BASE, exponent)
    wavelen = 2.0 * math.pi / inv_freq
    smooth = (ORIG_CONTEXT / wavelen - LOW_FREQ) / (HIGH_FREQ - LOW_FREQ)
    blended = (1.0 - smooth) * inv_freq / ROPE_FACTOR + smooth * inv_freq
    rope_freq = jnp.where(wavelen < ORIG_CONTEXT / HIGH_FREQ, inv_freq, jnp.where(wavelen > ORIG_CONTEXT / LOW_FREQ, inv_freq / ROPE_FACTOR, blended))
    angles = jnp.arange(SEQ, dtype=jnp.float32)[:, None] * rope_freq[None, :]
    return jnp.cos(angles), jnp.sin(angles)


def apply_rope(vec_in, cos_tab, sin_tab):
    half_dim = vec_in.shape[-1] // 2
    first_half = vec_in[..., :half_dim]
    second_half = vec_in[..., half_dim:]
    return jnp.concatenate([first_half * cos_tab - second_half * sin_tab, second_half * cos_tab + first_half * sin_tab], axis=-1)


def reference(x, lengths, k_buf, v_buf, w_qkv, w_o, w_gate_up, w_down, g_attn, g_mlp):
    packed = w_qkv.reshape(D, KV_HEADS, GROUP + 2, HEAD)
    w_q = packed[:, :, :GROUP, :].reshape(D, HEADS * HEAD)
    w_k = packed[:, :, GROUP, :].reshape(D, KV_HEADS * HEAD)
    w_v = packed[:, :, GROUP + 1, :].reshape(D, KV_HEADS * HEAD)
    gu_view = w_gate_up.reshape(D, TRAIN_TP, 2, FF_BLOCK)
    w_gate = gu_view[:, :, 0, :].reshape(D, FF)
    w_up = gu_view[:, :, 1, :].reshape(D, FF)
    cos_tab, sin_tab = rope_tables()
    positions = jnp.arange(SEQ)
    causal = positions[None, :] <= positions[:, None]

    def one_prompt(prompt_item):
        tokens, length = prompt_item
        x_normed = rms_norm(tokens, g_attn)
        queries = jnp.dot(x_normed, w_q, preferred_element_type=jnp.float32).astype(jnp.bfloat16).reshape(SEQ, KV_HEADS, GROUP, HEAD)
        keys_new = jnp.dot(x_normed, w_k, preferred_element_type=jnp.float32).astype(jnp.bfloat16).reshape(SEQ, KV_HEADS, HEAD)
        values = jnp.dot(x_normed, w_v, preferred_element_type=jnp.float32).astype(jnp.bfloat16).reshape(SEQ, KV_HEADS, HEAD)
        q_rot = apply_rope(queries.astype(jnp.float32), cos_tab[:, None, None, :], sin_tab[:, None, None, :]).astype(jnp.bfloat16)
        k_rot = apply_rope(keys_new.astype(jnp.float32), cos_tab[:, None, :], sin_tab[:, None, :]).astype(jnp.bfloat16)
        allowed = causal & (positions[None, :] < length)

        def one_group(kv_item):
            q_head, k_head, v_head = kv_item
            scores = jnp.einsum('qgd,sd->gqs', q_head.astype(jnp.float32), k_head.astype(jnp.float32)) * HEAD ** -0.5
            scores = jnp.where(allowed[None], scores, MASK_VALUE)
            attn_prob = jax.nn.softmax(scores, axis=-1).astype(jnp.bfloat16)
            return jnp.einsum('gqs,sd->qgd', attn_prob.astype(jnp.float32), v_head.astype(jnp.float32)).astype(jnp.bfloat16)

        per_group = lax.map(one_group, (q_rot.transpose(1, 0, 2, 3), k_rot.transpose(1, 0, 2), values.transpose(1, 0, 2)))
        attn_out = per_group.transpose(1, 0, 2, 3).reshape(SEQ, HEADS * HEAD)
        attn_proj = jnp.dot(attn_out, w_o, preferred_element_type=jnp.float32)
        hidden = (tokens.astype(jnp.float32) + attn_proj).astype(jnp.bfloat16)
        h_normed = rms_norm(hidden, g_mlp)
        gate_act = jnp.dot(h_normed, w_gate, preferred_element_type=jnp.float32).astype(jnp.bfloat16)
        up_act = jnp.dot(h_normed, w_up, preferred_element_type=jnp.float32).astype(jnp.bfloat16)
        mid_act = (jax.nn.silu(gate_act.astype(jnp.float32)) * up_act.astype(jnp.float32)).astype(jnp.bfloat16)
        layer_out = (hidden.astype(jnp.float32) + jnp.dot(mid_act, w_down, preferred_element_type=jnp.float32)).astype(jnp.bfloat16)
        return layer_out, k_rot, values

    layer_out, k_new, v_new = lax.map(one_prompt, (x, lengths))
    valid_pos = (positions[None, :] < lengths[:, None])[:, :, None, None]
    k_cache = jnp.where(valid_pos, k_new, k_buf)
    v_cache = jnp.where(valid_pos, v_new, v_buf)
    return (layer_out, k_cache, v_cache, w_q, w_k, w_v, w_o, w_gate, w_up, w_down)
```

```python
import functools
import math

import jax
import jax.numpy as jnp
from jax import lax
from jax.experimental import pallas as pl
from jax.experimental.pallas import tpu as pltpu
from jax.sharding import PartitionSpec as P


ROPE_BASE = 500000.0
ROPE_FACTOR = 8.0
LOW_FREQ = 1.0
HIGH_FREQ = 4.0
ORIG_CONTEXT = 8192.0
NORM_EPS = 1e-5
MASK_VALUE = -1e30
MESH = pl.DeviceIdType.MESH
F32 = jnp.float32
BF16 = jnp.bfloat16


def rms_norm(x_in, gain_vec):
    x_wide = x_in.astype(F32)
    mean_sq = jnp.mean(x_wide * x_wide, axis=-1, keepdims=True)
    return (x_wide * lax.rsqrt(mean_sq + NORM_EPS) * gain_vec.astype(F32)).astype(BF16)


def rope_tables(seq_len, head_dim):
    exponent = jnp.arange(head_dim // 2, dtype=F32) * (2.0 / head_dim)
    inv_freq = 1.0 / jnp.power(ROPE_BASE, exponent)
    wavelen = 2.0 * math.pi / inv_freq
    smooth = (ORIG_CONTEXT / wavelen - LOW_FREQ) / (HIGH_FREQ - LOW_FREQ)
    blended = (1.0 - smooth) * inv_freq / ROPE_FACTOR + smooth * inv_freq
    rope_freq = jnp.where(wavelen < ORIG_CONTEXT / HIGH_FREQ, inv_freq, jnp.where(wavelen > ORIG_CONTEXT / LOW_FREQ, inv_freq / ROPE_FACTOR, blended))
    angles = jnp.arange(seq_len, dtype=F32)[:, None] * rope_freq[None, :]
    return jnp.cos(angles), jnp.sin(angles)


def qkv_kernel(u_ref, w_ref, cos_ref, sin_ref, q_ref, k_ref, v_ref, wq_ref, wk_ref, wv_ref):
    hd = cos_ref.shape[1]
    for i in range(2):
        cols = slice(i * hd, (i + 1) * hd)
        wq_ref[:, cols] = w_ref[i, :, 0:hd]
        wk_ref[:, cols] = w_ref[i, :, hd:2 * hd]
        wv_ref[:, cols] = w_ref[i, :, 2 * hd:3 * hd]
    rows = u_ref.shape[0] // 2

    def half(r, carry):
        sl = pl.ds(pl.multiple_of(r * rows, rows), rows)
        u = u_ref[sl, :]
        cos, sin = cos_ref[sl, :], sin_ref[sl, :]
        for src, dst in ((wq_ref, q_ref), (wk_ref, k_ref)):
            prod = jnp.dot(u, src[...], preferred_element_type=F32).astype(BF16).astype(F32)
            for i in range(2):
                p = prod[:, i * hd:(i + 1) * hd]
                dst[sl, i * hd:(i + 1) * hd] = (p * cos + pltpu.roll(p, hd // 2, 1) * sin).astype(BF16)
        v_ref[sl, :] = jnp.dot(u, wv_ref[...], preferred_element_type=F32).astype(BF16)
        return carry

    lax.fori_loop(0, 2, half, 0)


def qkv_call(u, wg, cos, sin):
    seq, dim = u.shape
    heads, _, packed = wg.shape
    hd = packed // 3
    wide = 2 * hd
    act = jax.ShapeDtypeStruct((seq, heads * hd), BF16)
    wout = jax.ShapeDtypeStruct((dim, heads * hd), BF16)
    act_spec = pl.BlockSpec((seq, wide), lambda h: (0, h))
    w_spec = pl.BlockSpec((dim, wide), lambda h: (0, h))
    one = pl.Buffered(1)
    return pl.pallas_call(
        qkv_kernel,
        grid=(heads // 2,),
        in_specs=[
            pl.BlockSpec((seq, dim), lambda h: (0, 0), pipeline_mode=one),
            pl.BlockSpec((2, dim, packed), lambda h: (h, 0, 0)),
            pl.BlockSpec((seq, hd), lambda h: (0, 0), pipeline_mode=one),
            pl.BlockSpec((seq, hd), lambda h: (0, 0), pipeline_mode=one),
        ],
        out_specs=[act_spec, act_spec, act_spec, w_spec, w_spec, w_spec],
        out_shape=[act, act, act, wout, wout, wout],
        compiler_params=pltpu.CompilerParams(vmem_limit_bytes=60 << 20),
        cost_estimate=pl.CostEstimate(flops=2 * seq * dim * heads * packed, bytes_accessed=4 * dim * heads * packed, transcendentals=0),
        name="qkv",
    )(u, wg, cos, sin)


def attn_kernel(scale, block, len_ref, q_ref, k_ref, v_ref, o_ref):
    seq = q_ref.shape[0]
    length = len_ref[0]
    for i in range(seq // block):
        lo, hi = i * block, (i + 1) * block
        s = lax.dot_general(q_ref[lo:hi, :], k_ref[0:hi, :], (((1,), (1,)), ((), ())), preferred_element_type=F32) * scale
        row = lo + lax.broadcasted_iota(jnp.int32, s.shape, 0)
        col = lax.broadcasted_iota(jnp.int32, s.shape, 1)
        s = jnp.where((col <= row) & (col < length), s, MASK_VALUE)
        e = jnp.exp(s - jnp.max(s, axis=-1, keepdims=True))
        w = (e * (1.0 / jnp.sum(e, axis=-1, keepdims=True))).astype(BF16)
        o_ref[lo:hi, :] = jnp.dot(w, v_ref[0:hi, :], preferred_element_type=F32).astype(BF16)


def attn_call(length, q, k, v, hd):
    seq, width = q.shape
    heads = width // hd
    spec = pl.BlockSpec((seq, hd), lambda h: (0, h))
    return pl.pallas_call(
        functools.partial(attn_kernel, hd ** -0.5, 256),
        grid=(heads,),
        in_specs=[pl.BlockSpec(memory_space=pltpu.SMEM), spec, spec, spec],
        out_specs=spec,
        out_shape=jax.ShapeDtypeStruct((seq, width), BF16),
        compiler_params=pltpu.CompilerParams(vmem_limit_bytes=48 << 20),
        cost_estimate=pl.CostEstimate(flops=4 * seq * seq * width, bytes_accessed=8 * seq * width, transcendentals=seq * seq * heads),
        name="attn",
    )(length, q, k, v)


def gate_up_kernel(u_ref, w_ref, m_ref, wg_ref, wu_ref):
    ff = wg_ref.shape[1]
    wg_ref[0] = w_ref[0, 0:ff, :]
    wu_ref[0] = w_ref[0, ff:2 * ff, :]
    seq = u_ref.shape[0]
    tile = 256

    def part(j, carry):
        sl = pl.ds(pl.multiple_of(j * tile, tile), tile)
        both = lax.dot_general(w_ref[0], u_ref[sl, :], (((1,), (1,)), ((), ())), preferred_element_type=F32)
        gate = both[0:ff].astype(BF16).astype(F32)
        up = both[ff:2 * ff].astype(BF16).astype(F32)
        m_ref[0, :, sl] = (gate * jax.nn.sigmoid(gate) * up).astype(BF16)
        return carry

    lax.fori_loop(0, seq // tile, part, 0)


def gate_up_call(u, wg):
    seq, dim = u.shape
    blocks, rows, _ = wg.shape
    ff = rows // 2
    wout = jax.ShapeDtypeStruct((blocks, ff, dim), BF16)
    wspec = pl.BlockSpec((1, ff, dim), lambda h: (h, 0, 0))
    return pl.pallas_call(
        gate_up_kernel,
        grid=(blocks,),
        in_specs=[
            pl.BlockSpec((seq, dim), lambda h: (0, 0), pipeline_mode=pl.Buffered(1)),
            pl.BlockSpec((1, rows, dim), lambda h: (h, 0, 0)),
        ],
        out_specs=[pl.BlockSpec((1, ff, seq), lambda h: (h, 0, 0)), wspec, wspec],
        out_shape=[jax.ShapeDtypeStruct((blocks, ff, seq), BF16), wout, wout],
        compiler_params=pltpu.CompilerParams(vmem_limit_bytes=60 << 20),
        cost_estimate=pl.CostEstimate(flops=2 * seq * dim * blocks * rows, bytes_accessed=4 * dim * blocks * rows, transcendentals=seq * ff * blocks),
        name="gate_up",
    )(u, wg)


CHUNKS = 2
COPIES = 12


def sum_kernel(n, transposed, col0, a_ref, w_ref, res_ref, out_ref, a_buf, w_buf, res_buf, part, own, first, second, gath, in_sem, out_sem, send_sem, recv_sem):
    me = lax.axis_index("tpa")
    right, left, far = lax.rem(me + 1, n), lax.rem(me + n - 1, n), lax.rem(me + 2, n)
    order = (far, right, left, me)
    shard, width = own.shape
    half = width // 2
    rows = shard // CHUNKS
    tile = w_buf.shape[2]
    tiles = w_buf.shape[0]

    loads = []
    for s in range(n):
        span = pl.ds(pl.multiple_of(order[s] * shard, shard), shard)
        src = a_ref.at[:, span] if transposed else a_ref.at[span, :]
        loads.append(pltpu.make_async_copy(src, a_buf.at[s], in_sem.at[s]))
    wloads = [pltpu.make_async_copy(w_ref.at[:, t * tile:(t + 1) * tile], w_buf.at[t], in_sem.at[n + t]) for t in range(tiles)]
    mine = pl.ds(pl.multiple_of(me * shard, shard), shard)
    res_load = pltpu.make_async_copy(res_ref.at[mine, col0:col0 + width], res_buf, in_sem.at[n + tiles])
    loads[0].start()
    for c in wloads:
        c.start()
    for c in loads[1:]:
        c.start()
    res_load.start()

    barrier = pltpu.get_barrier_semaphore()
    for peer in (left, right):
        pl.semaphore_signal(barrier, inc=1, device_id={"tpa": peer}, device_id_type=MESH)
    pl.semaphore_wait(barrier, 2)

    A, B = slice(0, half), slice(half, width)

    def span_of(c):
        return slice(c * rows, (c + 1) * rows)

    def send(c, i, src, dst, peer):
        cp = pltpu.make_async_remote_copy(src_ref=src, dst_ref=dst, send_sem=send_sem.at[c, i], recv_sem=recv_sem.at[c, i], device_id={"tpa": peer}, device_id_type=MESH)
        cp.start()
        return cp

    dims = (((0,), (0,)), ((), ())) if transposed else (((1,), (0,)), ((), ()))

    def product(s, t):
        return lax.dot_general(a_buf[s], w_buf[t], dims, preferred_element_type=F32)

    sent = {}
    loads[0].wait()
    for t in range(tiles):
        wloads[t].wait()
        part[0, :, t * tile:(t + 1) * tile] = product(0, t).astype(BF16)
    for c in range(CHUNKS):
        r = span_of(c)
        sent[c, 0] = send(c, 0, part.at[0, r, A], first.at[0, r, :], right)
        sent[c, 1] = send(c, 1, part.at[0, r, B], first.at[1, r, :], left)
    for s in (1, 2):
        loads[s].wait()
        for t in range(tiles):
            part[s, :, t * tile:(t + 1) * tile] = product(s, t).astype(BF16)
        for c in range(CHUNKS):
            r = span_of(c)
            if s == 1:
                sent[c, 2] = send(c, 2, part.at[1, r, B], second.at[0, r, B], right)
            else:
                sent[c, 3] = send(c, 3, part.at[2, r, A], second.at[1, r, A], left)
    loads[3].wait()
    res_load.wait()
    for t in range(tiles):
        cols = slice(t * tile, (t + 1) * tile)
        own[:, cols] = res_buf[:, cols].astype(F32) + product(3, t)

    for c in range(CHUNKS):
        r = span_of(c)
        sent[c, 0].wait_recv()
        part[1, r, A] = (part[1, r, A].astype(F32) + first[0, r, :].astype(F32)).astype(BF16)
        sent[c, 4] = send(c, 4, part.at[1, r, A], second.at[0, r, A], right)
        sent[c, 1].wait_recv()
        part[2, r, B] = (part[2, r, B].astype(F32) + first[1, r, :].astype(F32)).astype(BF16)
        sent[c, 5] = send(c, 5, part.at[2, r, B], second.at[1, r, B], left)

    stores = []

    def store(c, slot, owner, i, cols):
        r = span_of(c)
        dst = out_ref.at[pl.ds(pl.multiple_of(owner * shard + c * rows, rows), rows), cols]
        cp = pltpu.make_async_copy(gath.at[slot, r, cols], dst, out_sem.at[c, i])
        cp.start()
        stores.append(cp)

    for c in range(CHUNKS):
        r = span_of(c)
        for i in (2, 4, 3, 5):
            sent[c, i].wait_recv()
        total = own[r, :] + second[0, r, :].astype(F32) + second[1, r, :].astype(F32)
        gath[0, r, :] = total.astype(BF16)
        sent[c, 6] = send(c, 6, gath.at[0, r, A], gath.at[1, r, A], right)
        sent[c, 7] = send(c, 7, gath.at[0, r, B], gath.at[2, r, B], left)
        sent[c, 8] = send(c, 8, gath.at[0, r, B], gath.at[1, r, B], right)
        sent[c, 9] = send(c, 9, gath.at[0, r, A], gath.at[2, r, A], left)
        store(c, 0, me, 0, slice(0, width))
    for c in range(CHUNKS):
        r = span_of(c)
        sent[c, 6].wait_recv()
        sent[c, 10] = send(c, 10, gath.at[1, r, A], gath.at[3, r, A], right)
        sent[c, 7].wait_recv()
        sent[c, 11] = send(c, 11, gath.at[2, r, B], gath.at[3, r, B], left)
        store(c, 1, left, 1, A)
        store(c, 2, right, 2, B)
    for c in range(CHUNKS):
        sent[c, 8].wait_recv()
        store(c, 1, left, 3, B)
        sent[c, 9].wait_recv()
        store(c, 2, right, 4, A)
    for c in range(CHUNKS):
        sent[c, 10].wait_recv()
        store(c, 3, far, 5, A)
        sent[c, 11].wait_recv()
        store(c, 3, far, 6, B)
    for cp in sent.values():
        cp.wait_send()
    for cp in stores:
        cp.wait()


def sum_call(n, a, w, res, col0, cid, transposed):
    depth, width = w.shape
    seq = res.shape[0]
    shard = seq // n
    tile = 512
    tiles = width // tile
    any_spec = pl.BlockSpec(memory_space=pl.ANY)
    a_shape = (n, depth, shard) if transposed else (n, shard, depth)
    return pl.pallas_call(
        functools.partial(sum_kernel, n, transposed, col0),
        in_specs=[any_spec] * 3,
        out_specs=any_spec,
        out_shape=jax.ShapeDtypeStruct((seq, width), BF16),
        scratch_shapes=[
            pltpu.VMEM(a_shape, BF16),
            pltpu.VMEM((tiles, depth, tile), BF16),
            pltpu.VMEM((shard, width), BF16),
            pltpu.VMEM((3, shard, width), BF16),
            pltpu.VMEM((shard, width), F32),
            pltpu.VMEM((2, shard, width // 2), BF16),
            pltpu.VMEM((2, shard, width), BF16),
            pltpu.VMEM((4, shard, width), BF16),
            pltpu.SemaphoreType.DMA((n + tiles + 1,)),
            pltpu.SemaphoreType.DMA((CHUNKS, 7)),
            pltpu.SemaphoreType.DMA((CHUNKS, COPIES)),
            pltpu.SemaphoreType.DMA((CHUNKS, COPIES)),
        ],
        compiler_params=pltpu.CompilerParams(collective_id=cid, has_side_effects=True, vmem_limit_bytes=62 << 20),
        cost_estimate=pl.CostEstimate(flops=2 * seq * depth * width + 130_000_000_000, bytes_accessed=2 * depth * width, transcendentals=0),
    )(a, w, res)


def copy_kernel(src_ref, dst_ref):
    dst_ref[...] = src_ref[...]


def copy_call(w):
    rows, width = w.shape
    block = rows // 8
    spec = pl.BlockSpec((block, width), lambda i: (i, 0))
    return pl.pallas_call(
        copy_kernel,
        grid=(rows // block,),
        in_specs=[spec],
        out_specs=spec,
        out_shape=jax.ShapeDtypeStruct((rows, width), w.dtype),
        compiler_params=pltpu.CompilerParams(vmem_limit_bytes=32 << 20),
        cost_estimate=pl.CostEstimate(flops=rows * width, bytes_accessed=4 * rows * width, transcendentals=0),
    )(w)


def solution(mesh):
    n_tpa = mesh.shape['tpa']
    assert n_tpa == 4

    def gather(w, tiled):
        return lax.all_gather(w, 'tpb', axis=0, tiled=tiled)

    def layer(x_loc, len_loc, k_buf, v_buf, w_qkv, w_o, w_gate_up, w_down, g_attn, g_mlp):
        seq, dim = x_loc.shape[1:]
        heads, hd = k_buf.shape[2:]
        half = dim // 2
        x = x_loc[0]
        qkv_g = gather(w_qkv, False)
        o_g = gather(w_o, True)
        gu_g = gather(w_gate_up.T, False)
        down_a = gather(w_down[:, :half], True)
        down_b = gather(w_down[:, half:], True)

        cos, sin = rope_tables(seq, hd)
        cos2 = jnp.concatenate([cos, cos], axis=-1)
        sin2 = jnp.concatenate([-sin, sin], axis=-1)
        u = rms_norm(x, g_attn)
        q, k, v, w_q, w_k, w_v = qkv_call(u, qkv_g, cos2, sin2)
        att = attn_call(len_loc, q, k, v, hd)
        hidden = sum_call(n_tpa, att, o_g, x, 0, 0, False)

        valid = (jnp.arange(seq) < len_loc[0])[:, None, None]
        k_cache = jnp.where(valid, k.reshape(seq, heads, hd), k_buf[0])[None]
        v_cache = jnp.where(valid, v.reshape(seq, heads, hd), v_buf[0])[None]
        o_out = copy_call(o_g)

        u2 = rms_norm(hidden, g_mlp)
        u2, k_cache, v_cache, o_out = lax.optimization_barrier((u2, k_cache, v_cache, o_out))
        m_t, gate_t, up_t = gate_up_call(u2, gu_g)
        ff = m_t.shape[0] * m_t.shape[1]
        m_t = m_t.reshape(ff, seq)
        y_a = sum_call(n_tpa, m_t, down_a, hidden, 0, 1, True)
        y_b = sum_call(n_tpa, m_t, down_b, hidden, half, 2, True)
        y = jnp.concatenate([y_a, y_b], axis=1)[None]
        down_a, down_b, _ = lax.optimization_barrier((down_a, down_b, y_a))
        down = jnp.concatenate([down_a, down_b], axis=1)
        return (y, k_cache, v_cache, w_q, w_k, w_v, o_out, gate_t.reshape(ff, dim).T, up_t.reshape(ff, dim).T, down)

    batch_spec = P(('part', 'tpb'), None, None)
    len_spec = P(('part', 'tpb'))
    cache_spec = P(('part', 'tpb'), None, 'tpa', None)
    train_cols = P('part', ('tpa', 'tpb'))
    train_rows = P(('part', 'tpa', 'tpb'), None)
    gain_spec = P('part')
    gen_cols = P('part', 'tpa')
    gen_rows = P(('part', 'tpa'), None)
    return jax.shard_map(layer, mesh=mesh, in_specs=(batch_spec, len_spec, cache_spec, cache_spec, train_cols, train_rows, train_cols, train_rows, gain_spec, gain_spec), out_specs=(batch_spec, cache_spec, cache_spec, gen_cols, gen_cols, gen_cols, gen_rows, gen_cols, gen_cols, gen_rows), check_vma=False)
```

```python
import functools
import math

import jax
import jax.numpy as jnp
from jax import lax
from jax.experimental import pallas as pl
from jax.experimental.pallas import tpu as pltpu
from jax.sharding import PartitionSpec as P


ROPE_BASE = 500000.0
ROPE_FACTOR = 8.0
LOW_FREQ = 1.0
HIGH_FREQ = 4.0
ORIG_CONTEXT = 8192.0
NORM_EPS = 1e-5
MASK_VALUE = -1e30
MESH = pl.DeviceIdType.MESH
F32 = jnp.float32
BF16 = jnp.bfloat16


def rope_tables(seq_len, head_dim):
    exponent = jnp.arange(head_dim // 2, dtype=F32) * (2.0 / head_dim)
    inv_freq = 1.0 / jnp.power(ROPE_BASE, exponent)
    wavelen = 2.0 * math.pi / inv_freq
    smooth = (ORIG_CONTEXT / wavelen - LOW_FREQ) / (HIGH_FREQ - LOW_FREQ)
    blended = (1.0 - smooth) * inv_freq / ROPE_FACTOR + smooth * inv_freq
    rope_freq = jnp.where(wavelen < ORIG_CONTEXT / HIGH_FREQ, inv_freq, jnp.where(wavelen > ORIG_CONTEXT / LOW_FREQ, inv_freq / ROPE_FACTOR, blended))
    angles = jnp.arange(seq_len, dtype=F32)[:, None] * rope_freq[None, :]
    return jnp.cos(angles), jnp.sin(angles)


PIECES = 4


def gather_qkv_kernel(chips, x_ref, gain_ref, w_ref, cos_ref, sin_ref, q_ref, k_ref, v_ref, all_ref, u_buf, w_buf, gain_buf, cos_buf, sin_buf, acc, in_sem, out_sem, send_sem, recv_sem):
    here = lax.axis_index("tpb")
    chip, core = here // 2, lax.rem(here, 2)
    right, left, far = lax.rem(chip + 1, chips), lax.rem(chip + chips - 1, chips), lax.rem(chip + 2, chips)
    other = 1 - core
    mate = 2 * chip + other
    dim, packed = w_ref.shape
    hd = packed // 3
    seq = x_ref.shape[0]
    depth = dim // PIECES
    mid = dim // 2
    A, B = slice(0, mid), slice(mid, dim)

    loads = [
        pltpu.make_async_copy(w_ref, w_buf.at[here], in_sem.at[0]),
        pltpu.make_async_copy(x_ref, u_buf, in_sem.at[1]),
        pltpu.make_async_copy(cos_ref, cos_buf, in_sem.at[2]),
        pltpu.make_async_copy(sin_ref, sin_buf, in_sem.at[3]),
        pltpu.make_async_copy(gain_ref, gain_buf, in_sem.at[4]),
    ]
    barrier = pltpu.get_barrier_semaphore()
    for peer in (2 * left + core, 2 * right + core, mate):
        pl.semaphore_signal(barrier, inc=1, device_id={"tpb": peer}, device_id_type=MESH)
    pl.semaphore_wait(barrier, 3)

    def send(i, src, slot, rows, peer):
        cp = pltpu.make_async_remote_copy(src_ref=src, dst_ref=w_buf.at[slot, rows, :], send_sem=send_sem.at[i], recv_sem=recv_sem.at[i], device_id={"tpb": peer}, device_id_type=MESH)
        cp.start()
        return cp

    def piece(j):
        return slice(j * depth, (j + 1) * depth)

    sent = {}
    to_right, to_left = 2 * right + core, 2 * left + core
    for j in range(PIECES):
        jl = (j + PIECES // 2) % PIECES
        sent[j] = send(j, w_ref.at[piece(j), :], here, piece(j), to_right)
        sent[4 + jl] = send(4 + jl, w_ref.at[piece(jl), :], here, piece(jl), to_left)
    sent[8] = send(8, w_ref, here, slice(0, dim), mate)
    for c in loads:
        c.start()

    rows = seq // 2

    def finish(prod, slot, sl):
        cos, sin = cos_buf[sl, :], sin_buf[sl, :]
        cos, sin = jnp.concatenate([cos, cos], axis=1), jnp.concatenate([-sin, sin], axis=1)
        for n, dst in ((0, q_ref), (1, k_ref)):
            p = prod[:, n * hd:(n + 1) * hd].astype(BF16).astype(F32)
            dst[slot, sl, :] = (p * cos + pltpu.roll(p, hd // 2, 1) * sin).astype(BF16)
        v_ref[slot, sl, :] = prod[:, 2 * hd:].astype(BF16)

    def over(slots, fn):
        def body(i, carry):
            sl = pl.ds(pl.multiple_of(lax.rem(i, 2) * rows, rows), rows)
            fn(i // 2, jnp.where(i < 2, slots[0], slots[1]), sl)
            return carry

        lax.fori_loop(0, 4, body, 0)

    def part_of(slot, sl, j):
        return jnp.dot(u_buf[sl, piece(j)], w_buf[slot, piece(j), :], preferred_element_type=F32)

    def project(slots):
        over(slots, lambda n, slot, sl: finish(jnp.dot(u_buf[sl, :], w_buf[slot], preferred_element_type=F32), slot, sl))

    def project_first(slots):
        def fn(n, slot, sl):
            acc[n, sl, :] = part_of(slot, sl, 0) + part_of(slot, sl, 2)

        over(slots, fn)

    def project_last(slots):
        over(slots, lambda n, slot, sl: finish(acc[n, sl, :] + part_of(slot, sl, 1) + part_of(slot, sl, 3), slot, sl))

    stores = []

    def store(slot, i):
        cp = pltpu.make_async_copy(w_buf.at[slot], all_ref.at[slot], out_sem.at[i])
        cp.start()
        stores.append(cp)

    for c in loads:
        c.wait()
    norm_rows = 64
    gain = gain_buf[...].astype(F32).reshape(1, dim)

    def norm(i, carry):
        sl = pl.ds(pl.multiple_of(i * norm_rows, norm_rows), norm_rows)
        x = u_buf[sl, :].astype(F32)
        mean_sq = jnp.sum(x * x, axis=-1, keepdims=True) * (1.0 / dim)
        u_buf[sl, :] = (x * lax.rsqrt(mean_sq + NORM_EPS) * gain).astype(BF16)
        return carry

    lax.fori_loop(0, seq // norm_rows, norm, 0)
    sent[8].wait_recv()
    store(here, 0)
    store(mate, 1)
    project((here, mate))
    ls, rs, fs = to_left, to_right, 2 * far + core
    for j in (0, 1):
        sent[j].wait_recv()
        sent[9 + j] = send(9 + j, w_buf.at[ls, piece(j), :], ls, piece(j), to_right)
        sent[4 + 2 + j].wait_recv()
        sent[11 + j] = send(11 + j, w_buf.at[rs, piece(2 + j), :], rs, piece(2 + j), to_left)
    sent[13] = send(13, w_buf.at[ls, A, :], ls, A, mate)
    sent[14] = send(14, w_buf.at[rs, B, :], rs, B, mate)
    for j in (0, 1):
        sent[2 + j].wait_recv()
        sent[4 + j].wait_recv()
    sent[15] = send(15, w_buf.at[ls, B, :], ls, B, mate)
    sent[16] = send(16, w_buf.at[rs, A, :], rs, A, mate)
    store(ls, 2)
    store(rs, 3)
    project((ls, rs))
    for i in (13, 14, 15, 16):
        sent[i].wait_recv()
    store(2 * left + other, 4)
    store(2 * right + other, 5)
    project((2 * left + other, 2 * right + other))
    last = (fs, 2 * far + other)
    for j in (0, 1):
        sent[9 + j].wait_recv()
        sent[17 + 2 * j] = send(17 + 2 * j, w_buf.at[fs, piece(j), :], fs, piece(j), mate)
        sent[11 + j].wait_recv()
        sent[18 + 2 * j] = send(18 + 2 * j, w_buf.at[fs, piece(2 + j), :], fs, piece(2 + j), mate)
        sent[17 + 2 * j].wait_recv()
        sent[18 + 2 * j].wait_recv()
        if j == 0:
            project_first(last)
    store(last[0], 6)
    store(last[1], 7)
    project_last(last)
    for cp in sent.values():
        cp.wait_send()
    for cp in stores:
        cp.wait()


def gather_qkv_call(n, x, gain, w, cos, sin):
    seq, dim = x.shape
    packed = w.shape[1]
    hd = packed // 3
    act = jax.ShapeDtypeStruct((n, seq, hd), BF16)
    any_spec = pl.BlockSpec(memory_space=pl.ANY)
    vmem = pl.BlockSpec(memory_space=pltpu.VMEM)
    return pl.pallas_call(
        functools.partial(gather_qkv_kernel, n // 2),
        in_specs=[any_spec] * 5,
        out_specs=[vmem, vmem, vmem, any_spec],
        out_shape=[act, act, act, jax.ShapeDtypeStruct((n, dim, packed), BF16)],
        scratch_shapes=[
            pltpu.VMEM((seq, dim), BF16),
            pltpu.VMEM((n, dim, packed), BF16),
            pltpu.VMEM((dim,), BF16),
            pltpu.VMEM((seq, hd // 2), F32),
            pltpu.VMEM((seq, hd // 2), F32),
            pltpu.VMEM((2, seq, packed), F32),
            pltpu.SemaphoreType.DMA((5,)),
            pltpu.SemaphoreType.DMA((n,)),
            pltpu.SemaphoreType.DMA((21,)),
            pltpu.SemaphoreType.DMA((21,)),
        ],
        compiler_params=pltpu.CompilerParams(collective_id=3, has_side_effects=True, vmem_limit_bytes=62 << 20),
        cost_estimate=pl.CostEstimate(flops=120_000_000_000, bytes_accessed=4 * dim * n * packed, transcendentals=0),
        name="gather_qkv",
    )(x, gain, w, cos, sin)


def unpack_kernel(w_ref, wq_ref, wk_ref, wv_ref):
    hd = w_ref.shape[2] // 3
    for i in range(2):
        cols = slice(i * hd, (i + 1) * hd)
        wq_ref[:, cols] = w_ref[i, :, 0:hd]
        wk_ref[:, cols] = w_ref[i, :, hd:2 * hd]
        wv_ref[:, cols] = w_ref[i, :, 2 * hd:3 * hd]


def unpack_call(wg):
    heads, dim, packed = wg.shape
    hd = packed // 3
    block = dim // 2
    wout = jax.ShapeDtypeStruct((dim, heads * hd), BF16)
    w_spec = pl.BlockSpec((block, 2 * hd), lambda h, r: (r, h))
    return pl.pallas_call(
        unpack_kernel,
        grid=(heads // 2, dim // block),
        in_specs=[pl.BlockSpec((2, block, packed), lambda h, r: (h, r, 0))],
        out_specs=[w_spec, w_spec, w_spec],
        out_shape=[wout, wout, wout],
        compiler_params=pltpu.CompilerParams(vmem_limit_bytes=62 << 20),
        cost_estimate=pl.CostEstimate(flops=dim * heads * packed, bytes_accessed=4 * dim * heads * packed, transcendentals=0),
        name="unpack",
    )(wg)


def gate_up_kernel(u_ref, w_ref, m_ref, wg_ref, wu_ref):
    ff = wg_ref.shape[1]
    wg_ref[0] = w_ref[0, 0:ff, :]
    wu_ref[0] = w_ref[0, ff:2 * ff, :]
    seq = u_ref.shape[0]
    tile = 1024

    def part(j, carry):
        sl = pl.ds(pl.multiple_of(j * tile, tile), tile)
        both = lax.dot_general(w_ref[0], u_ref[sl, :], (((1,), (1,)), ((), ())), preferred_element_type=F32)
        gate = both[0:ff].astype(BF16).astype(F32)
        up = both[ff:2 * ff].astype(BF16).astype(F32)
        m_ref[0, :, sl] = (gate * jax.nn.sigmoid(gate) * up).astype(BF16)
        return carry

    lax.fori_loop(0, seq // tile, part, 0)


def gate_up_call(u, wg):
    seq, dim = u.shape
    blocks, rows, _ = wg.shape
    ff = rows // 2
    wout = jax.ShapeDtypeStruct((blocks, ff, dim), BF16)
    wspec = pl.BlockSpec((1, ff, dim), lambda h: (h, 0, 0))
    return pl.pallas_call(
        gate_up_kernel,
        grid=(blocks,),
        in_specs=[
            pl.BlockSpec((seq, dim), lambda h: (0, 0), pipeline_mode=pl.Buffered(1)),
            pl.BlockSpec((1, rows, dim), lambda h: (h, 0, 0)),
        ],
        out_specs=[pl.BlockSpec((1, ff, seq), lambda h: (h, 0, 0)), wspec, wspec],
        out_shape=[jax.ShapeDtypeStruct((blocks, ff, seq), BF16), wout, wout],
        compiler_params=pltpu.CompilerParams(vmem_limit_bytes=60 << 20),
        cost_estimate=pl.CostEstimate(flops=2 * seq * dim * blocks * rows, bytes_accessed=4 * dim * blocks * rows, transcendentals=seq * ff * blocks),
        name="gate_up",
    )(u, wg)


CHUNKS = 2
COPIES = 12


def sum_kernel(n, transposed, col0, *refs):
    if transposed:
        a_ref, w_ref, res_ref, out_ref, *scratch = refs
    else:
        len_ref, q_ref, k_ref, v_ref, gain_ref, w_ref, res_ref, out_ref, norm_ref, norm_buf, norm_sem, *scratch = refs
    a_buf, w_buf, res_buf, part, own, first, second, gath, in_sem, out_sem, send_sem, recv_sem = scratch
    me = lax.axis_index("tpa")
    right, left, far = lax.rem(me + 1, n), lax.rem(me + n - 1, n), lax.rem(me + 2, n)
    order = (far, right, left, me)
    shard, width = own.shape
    half = width // 2
    rows = shard // CHUNKS
    tile = w_buf.shape[2]
    tiles = w_buf.shape[0]

    loads = []
    if transposed:
        for s in range(n):
            span = pl.ds(pl.multiple_of(order[s] * shard, shard), shard)
            loads.append(pltpu.make_async_copy(a_ref.at[:, span], a_buf.at[s], in_sem.at[s]))
    wloads = [pltpu.make_async_copy(w_ref.at[:, t * tile:(t + 1) * tile], w_buf.at[t], in_sem.at[n + t]) for t in range(tiles)]
    mine = pl.ds(pl.multiple_of(me * shard, shard), shard)
    res_load = pltpu.make_async_copy(res_ref.at[mine, col0:col0 + width], res_buf, in_sem.at[n + tiles])
    for c in loads[:1] + wloads + loads[1:] + [res_load]:
        c.start()

    barrier = pltpu.get_barrier_semaphore()
    for peer in (left, right):
        pl.semaphore_signal(barrier, inc=1, device_id={"tpa": peer}, device_id_type=MESH)
    pl.semaphore_wait(barrier, 2)

    A, B = slice(0, half), slice(half, width)

    def span_of(c):
        return slice(c * rows, (c + 1) * rows)

    def send(c, i, src, dst, peer):
        cp = pltpu.make_async_remote_copy(src_ref=src, dst_ref=dst, send_sem=send_sem.at[c, i], recv_sem=recv_sem.at[c, i], device_id={"tpa": peer}, device_id_type=MESH)
        cp.start()
        return cp

    dims = (((0,), (0,)), ((), ())) if transposed else (((1,), (0,)), ((), ()))

    def ready(s):
        if transposed:
            loads[s].wait()
            return
        heads, _, hd = k_ref.shape
        base = pl.multiple_of(order[s] * shard, shard)
        length = len_ref[0]

        def head(h, carry):
            q = q_ref[h, pl.ds(base, shard), :]
            sc = lax.dot_general(q, k_ref[h], (((1,), (1,)), ((), ())), preferred_element_type=F32) * hd ** -0.5
            row = base + lax.broadcasted_iota(jnp.int32, sc.shape, 0)
            col = lax.broadcasted_iota(jnp.int32, sc.shape, 1)
            sc = jnp.where((col <= row) & (col < length), sc, MASK_VALUE)
            e = jnp.exp(sc - jnp.max(sc, axis=-1, keepdims=True))
            prob = (e * (1.0 / jnp.sum(e, axis=-1, keepdims=True))).astype(BF16)
            out = jnp.dot(prob, v_ref[h], preferred_element_type=F32).astype(BF16)
            a_buf[s, :, pl.ds(pl.multiple_of(h * hd, hd), hd)] = out
            return carry

        lax.fori_loop(0, heads, head, 0)

    def product(s, t):
        return lax.dot_general(a_buf[s], w_buf[t], dims, preferred_element_type=F32)

    def tile_loop(lo, hi, fn):
        def body(t, carry):
            fn(t, pl.ds(pl.multiple_of(t * tile, tile), tile))
            return carry

        lax.fori_loop(lo, hi, body, 0)

    def fill(s, lo, hi):
        def fn(t, cols):
            part[s, :, cols] = product(s, t).astype(BF16)

        tile_loop(lo, hi, fn)

    sent = {}
    mid, quarter = tiles // 2, tiles // 4
    ready(0)
    for part_no in (0, 2, 1, 3):
        for t in range(part_no * quarter, (part_no + 1) * quarter):
            wloads[t].wait()
        fill(0, part_no * quarter, (part_no + 1) * quarter)
        side, c = divmod(part_no, 2)
        wide = width // 4
        src = part.at[0, :, part_no * wide:(part_no + 1) * wide]
        dst = first.at[side, :, c * wide:(c + 1) * wide]
        sent[c, side] = send(c, side, src, dst, (right, left)[side])
    ready(1)
    fill(1, mid, tiles)
    for c in range(CHUNKS):
        r = span_of(c)
        sent[c, 2] = send(c, 2, part.at[1, r, B], second.at[0, r, B], right)
    ready(2)
    fill(2, 0, mid)
    for c in range(CHUNKS):
        r = span_of(c)
        sent[c, 3] = send(c, 3, part.at[2, r, A], second.at[1, r, A], left)
    fill(1, 0, mid)
    fill(2, mid, tiles)
    ready(3)
    res_load.wait()

    def mine_too(t, cols):
        own[:, cols] = res_buf[:, cols].astype(F32) + product(3, t)

    tile_loop(0, tiles, mine_too)

    for c in range(CHUNKS):
        r = span_of(c)
        if c == 0:
            sent[0, 0].wait_recv()
            sent[1, 0].wait_recv()
        part[1, r, A] = (part[1, r, A].astype(F32) + first[0, r, :].astype(F32)).astype(BF16)
        sent[c, 4] = send(c, 4, part.at[1, r, A], second.at[0, r, A], right)
        if c == 0:
            sent[0, 1].wait_recv()
            sent[1, 1].wait_recv()
        part[2, r, B] = (part[2, r, B].astype(F32) + first[1, r, :].astype(F32)).astype(BF16)
        sent[c, 5] = send(c, 5, part.at[2, r, B], second.at[1, r, B], left)

    stores = []

    def normed(c, slot, owner):
        if transposed:
            return
        gain = gain_ref[...].astype(F32).reshape(1, width)
        step = 16

        def body(i, carry):
            sl = pl.ds(pl.multiple_of(c * rows + i * step, step), step)
            x = gath[slot, sl, :].astype(F32)
            mean_sq = jnp.sum(x * x, axis=-1, keepdims=True) * (1.0 / width)
            norm_buf[slot, sl, :] = (x * lax.rsqrt(mean_sq + NORM_EPS) * gain).astype(BF16)
            return carry

        lax.fori_loop(0, rows // step, body, 0)
        dst = norm_ref.at[pl.ds(pl.multiple_of(owner * shard + c * rows, rows), rows), :]
        cp = pltpu.make_async_copy(norm_buf.at[slot, span_of(c), :], dst, norm_sem.at[c, slot])
        cp.start()
        stores.append(cp)

    def store(c, slot, owner, i, cols):
        r = span_of(c)
        dst = out_ref.at[pl.ds(pl.multiple_of(owner * shard + c * rows, rows), rows), cols]
        cp = pltpu.make_async_copy(gath.at[slot, r, cols], dst, out_sem.at[c, i])
        cp.start()
        stores.append(cp)

    for c in range(CHUNKS):
        r = span_of(c)
        for i in (2, 4, 3, 5):
            sent[c, i].wait_recv()
        total = own[r, :] + second[0, r, :].astype(F32) + second[1, r, :].astype(F32)
        gath[0, r, :] = total.astype(BF16)
        sent[c, 6] = send(c, 6, gath.at[0, r, A], gath.at[1, r, A], right)
        sent[c, 7] = send(c, 7, gath.at[0, r, B], gath.at[2, r, B], left)
        sent[c, 8] = send(c, 8, gath.at[0, r, B], gath.at[1, r, B], right)
        sent[c, 9] = send(c, 9, gath.at[0, r, A], gath.at[2, r, A], left)
        store(c, 0, me, 0, slice(0, width))
    for c in range(CHUNKS):
        normed(c, 0, me)
    for c in range(CHUNKS):
        r = span_of(c)
        sent[c, 6].wait_recv()
        sent[c, 10] = send(c, 10, gath.at[1, r, A], gath.at[3, r, A], right)
        sent[c, 7].wait_recv()
        sent[c, 11] = send(c, 11, gath.at[2, r, B], gath.at[3, r, B], left)
        store(c, 1, left, 1, A)
        store(c, 2, right, 2, B)
    for c in range(CHUNKS):
        sent[c, 8].wait_recv()
        store(c, 1, left, 3, B)
        normed(c, 1, left)
        sent[c, 9].wait_recv()
        store(c, 2, right, 4, A)
        normed(c, 2, right)
    for c in range(CHUNKS):
        sent[c, 10].wait_recv()
        store(c, 3, far, 5, A)
        sent[c, 11].wait_recv()
        store(c, 3, far, 6, B)
        normed(c, 3, far)
    for cp in sent.values():
        cp.wait_send()
    for cp in stores:
        cp.wait()


def sum_call(n, a, w, res, col0, cid, transposed):
    depth, width = w.shape
    seq = res.shape[0]
    shard = seq // n
    tile = 512
    tiles = width // tile
    assert CHUNKS == 2 and tiles % 4 == 0
    any_spec = pl.BlockSpec(memory_space=pl.ANY)
    a_shape = (n, depth, shard) if transposed else (n, shard, depth)
    vmem = pl.BlockSpec(memory_space=pltpu.VMEM)
    head_specs = [any_spec] if transposed else [pl.BlockSpec(memory_space=pltpu.SMEM), vmem, vmem, vmem, vmem]
    out = jax.ShapeDtypeStruct((seq, width), BF16)
    norm_scratch = [] if transposed else [pltpu.VMEM((4, shard, width), BF16), pltpu.SemaphoreType.DMA((CHUNKS, 4))]
    return pl.pallas_call(
        functools.partial(sum_kernel, n, transposed, col0),
        in_specs=head_specs + [any_spec] * 2,
        out_specs=any_spec if transposed else [any_spec] * 2,
        out_shape=out if transposed else [out] * 2,
        scratch_shapes=norm_scratch + [
            pltpu.VMEM(a_shape, BF16),
            pltpu.VMEM((tiles, depth, tile), BF16),
            pltpu.VMEM((shard, width), BF16),
            pltpu.VMEM((3, shard, width), BF16),
            pltpu.VMEM((shard, width), F32),
            pltpu.VMEM((2, shard, width // 2), BF16),
            pltpu.VMEM((2, shard, width), BF16),
            pltpu.VMEM((4, shard, width), BF16),
            pltpu.SemaphoreType.DMA((n + tiles + 1,)),
            pltpu.SemaphoreType.DMA((CHUNKS, 7)),
            pltpu.SemaphoreType.DMA((CHUNKS, COPIES)),
            pltpu.SemaphoreType.DMA((CHUNKS, COPIES)),
        ],
        compiler_params=pltpu.CompilerParams(collective_id=cid, has_side_effects=True, vmem_limit_bytes=62 << 20),
        cost_estimate=pl.CostEstimate(flops=2 * seq * depth * width + 130_000_000_000, bytes_accessed=2 * depth * width, transcendentals=0),
    )(*a, w, res)


def copy_kernel(src_ref, dst_ref):
    dst_ref[...] = src_ref[...]


def copy_call(w):
    rows, width = w.shape
    block = rows // 8
    spec = pl.BlockSpec((block, width), lambda i: (i, 0))
    return pl.pallas_call(
        copy_kernel,
        grid=(rows // block,),
        in_specs=[spec],
        out_specs=spec,
        out_shape=jax.ShapeDtypeStruct((rows, width), w.dtype),
        compiler_params=pltpu.CompilerParams(vmem_limit_bytes=62 << 20),
        cost_estimate=pl.CostEstimate(flops=rows * width, bytes_accessed=4 * rows * width, transcendentals=0),
    )(w)


def finish_kernel(ya_ref, yb_ref, da_ref, db_ref, y_ref, d_ref):
    half = ya_ref.shape[1]
    y_ref[:, :half] = ya_ref[...]
    y_ref[:, half:] = yb_ref[...]
    d_ref[:, :half] = da_ref[...]
    d_ref[:, half:] = db_ref[...]


def finish_call(y_a, y_b, d_a, d_b):
    steps = 8
    seq, half = y_a.shape
    ff = d_a.shape[0]

    def spec(rows, width):
        return pl.BlockSpec((rows // steps, width), lambda i: (i, 0))

    return pl.pallas_call(
        finish_kernel,
        grid=(steps,),
        in_specs=[spec(seq, half), spec(seq, half), spec(ff, half), spec(ff, half)],
        out_specs=[spec(seq, 2 * half), spec(ff, 2 * half)],
        out_shape=[jax.ShapeDtypeStruct((seq, 2 * half), BF16), jax.ShapeDtypeStruct((ff, 2 * half), BF16)],
        compiler_params=pltpu.CompilerParams(vmem_limit_bytes=62 << 20),
        cost_estimate=pl.CostEstimate(flops=ff * half, bytes_accessed=8 * (seq + ff) * half, transcendentals=0),
        name="finish",
    )(y_a, y_b, d_a, d_b)


def solution(mesh):
    n_tpa = mesh.shape['tpa']
    assert n_tpa == 4

    def gather(w, tiled):
        return lax.all_gather(w, 'tpb', axis=0, tiled=tiled)

    def layer(x_loc, len_loc, k_buf, v_buf, w_qkv, w_o, w_gate_up, w_down, g_attn, g_mlp):
        seq, dim = x_loc.shape[1:]
        _, hd = k_buf.shape[2:]
        half = dim // 2
        x = x_loc[0]
        cos, sin = rope_tables(seq, hd)
        o_g = gather(w_o, True)
        q, k, v, qkv_g = gather_qkv_call(mesh.shape['tpb'], x, g_attn, w_qkv, cos, sin)
        gu_in, d_in, q = lax.optimization_barrier((w_gate_up.T, w_down, q))
        gu_g = gather(gu_in, False)
        down_a = gather(d_in[:, :half], True)
        down_b = gather(d_in[:, half:], True)
        hidden, u2 = sum_call(n_tpa, (len_loc, q, k, v, g_mlp), o_g, x, 0, 0, False)

        hidden, u2, k, v, o_g, qkv_g = lax.optimization_barrier((hidden, u2, k, v, o_g, qkv_g))
        valid = (jnp.arange(seq) < len_loc[0])[:, None, None]
        k_cache = jnp.where(valid, k.transpose(1, 0, 2), k_buf[0])[None]
        v_cache = jnp.where(valid, v.transpose(1, 0, 2), v_buf[0])[None]
        o_out = copy_call(o_g)
        w_q, w_k, w_v = unpack_call(qkv_g)
        u2, k_cache, v_cache, o_out, w_q, w_k, w_v = lax.optimization_barrier((u2, k_cache, v_cache, o_out, w_q, w_k, w_v))
        m_t, gate_t, up_t = gate_up_call(u2, gu_g)
        ff = m_t.shape[0] * m_t.shape[1]
        m_t = m_t.reshape(ff, seq)
        y_a = sum_call(n_tpa, (m_t,), down_a, hidden, 0, 1, True)
        y_b = sum_call(n_tpa, (m_t,), down_b, hidden, half, 2, True)
        y, down = finish_call(y_a, y_b, down_a, down_b)
        return (y[None], k_cache, v_cache, w_q, w_k, w_v, o_out, gate_t.reshape(ff, dim).T, up_t.reshape(ff, dim).T, down)

    batch_spec = P(('part', 'tpb'), None, None)
    len_spec = P(('part', 'tpb'))
    cache_spec = P(('part', 'tpb'), None, 'tpa', None)
    train_cols = P('part', ('tpa', 'tpb'))
    train_rows = P(('part', 'tpa', 'tpb'), None)
    gain_spec = P('part')
    gen_cols = P('part', 'tpa')
    gen_rows = P(('part', 'tpa'), None)
    return jax.shard_map(layer, mesh=mesh, in_specs=(batch_spec, len_spec, cache_spec, cache_spec, train_cols, train_rows, train_cols, train_rows, gain_spec, gain_spec), out_specs=(batch_spec, cache_spec, cache_spec, gen_cols, gen_cols, gen_cols, gen_rows, gen_cols, gen_cols, gen_rows), check_vma=False)
```

```python
import functools
import math

import jax
import jax.numpy as jnp
from jax import lax
from jax.experimental import pallas as pl
from jax.experimental.pallas import tpu as pltpu
from jax.sharding import PartitionSpec as P


ROPE_BASE = 500000.0
ROPE_FACTOR = 8.0
LOW_FREQ = 1.0
HIGH_FREQ = 4.0
ORIG_CONTEXT = 8192.0
NORM_EPS = 1e-5
MASK_VALUE = -1e30
MESH = pl.DeviceIdType.MESH
F32 = jnp.float32
BF16 = jnp.bfloat16


def rope_tables(seq_len, head_dim):
    exponent = jnp.arange(head_dim // 2, dtype=F32) * (2.0 / head_dim)
    inv_freq = 1.0 / jnp.power(ROPE_BASE, exponent)
    wavelen = 2.0 * math.pi / inv_freq
    smooth = (ORIG_CONTEXT / wavelen - LOW_FREQ) / (HIGH_FREQ - LOW_FREQ)
    blended = (1.0 - smooth) * inv_freq / ROPE_FACTOR + smooth * inv_freq
    rope_freq = jnp.where(wavelen < ORIG_CONTEXT / HIGH_FREQ, inv_freq, jnp.where(wavelen > ORIG_CONTEXT / LOW_FREQ, inv_freq / ROPE_FACTOR, blended))
    angles = jnp.arange(seq_len, dtype=F32)[:, None] * rope_freq[None, :]
    return jnp.cos(angles), jnp.sin(angles)


PIECES = 8


def gather_qkv_kernel(chips, x_ref, gain_ref, w_ref, cos_ref, sin_ref, q_ref, k_ref, v_ref, all_ref, u_buf, w_buf, gain_buf, cos_buf, sin_buf, acc, in_sem, out_sem, send_sem, recv_sem):
    here = lax.axis_index("tpb")
    chip, core = here // 2, lax.rem(here, 2)
    right, left, far = lax.rem(chip + 1, chips), lax.rem(chip + chips - 1, chips), lax.rem(chip + 2, chips)
    other = 1 - core
    mate = 2 * chip + other
    dim, packed = w_ref.shape
    hd = packed // 3
    seq = x_ref.shape[0]
    depth = dim // PIECES
    mid = dim // 2
    A, B = slice(0, mid), slice(mid, dim)

    loads = [
        pltpu.make_async_copy(w_ref, w_buf.at[here], in_sem.at[0]),
        pltpu.make_async_copy(x_ref, u_buf, in_sem.at[1]),
        pltpu.make_async_copy(cos_ref, cos_buf, in_sem.at[2]),
        pltpu.make_async_copy(sin_ref, sin_buf, in_sem.at[3]),
        pltpu.make_async_copy(gain_ref, gain_buf, in_sem.at[4]),
    ]
    barrier = pltpu.get_barrier_semaphore()
    for peer in (2 * left + core, 2 * right + core, mate):
        pl.semaphore_signal(barrier, inc=1, device_id={"tpb": peer}, device_id_type=MESH)
    pl.semaphore_wait(barrier, 3)

    def send(i, src, slot, rows, peer):
        cp = pltpu.make_async_remote_copy(src_ref=src, dst_ref=w_buf.at[slot, rows, :], send_sem=send_sem.at[i], recv_sem=recv_sem.at[i], device_id={"tpb": peer}, device_id_type=MESH)
        cp.start()
        return cp

    def piece(j):
        return slice(j * depth, (j + 1) * depth)

    sent = {}
    to_right, to_left = 2 * right + core, 2 * left + core
    few = PIECES // 2
    own_left, own_mate, on_right, on_left, sides, ends = PIECES, 2 * PIECES, 2 * PIECES + 1, 2 * PIECES + 1 + few, 3 * PIECES + 1, 3 * PIECES + 5
    for j in range(PIECES):
        jl = (j + few) % PIECES
        sent[j] = send(j, w_ref.at[piece(j), :], here, piece(j), to_right)
        sent[own_left + jl] = send(own_left + jl, w_ref.at[piece(jl), :], here, piece(jl), to_left)
    sent[own_mate] = send(own_mate, w_ref, here, slice(0, dim), mate)
    for c in loads:
        c.start()

    rows = seq // 2

    def finish(prod, slot, sl):
        cos, sin = cos_buf[sl, :], sin_buf[sl, :]
        cos, sin = jnp.concatenate([cos, cos], axis=1), jnp.concatenate([-sin, sin], axis=1)
        for n, dst in ((0, q_ref), (1, k_ref)):
            p = prod[:, n * hd:(n + 1) * hd].astype(BF16).astype(F32)
            dst[slot, sl, :] = (p * cos + pltpu.roll(p, hd // 2, 1) * sin).astype(BF16)
        v_ref[slot, sl, :] = prod[:, 2 * hd:].astype(BF16)

    def over(slots, fn):
        def body(i, carry):
            sl = pl.ds(pl.multiple_of(lax.rem(i, 2) * rows, rows), rows)
            fn(i // 2, jnp.where(i < 2, slots[0], slots[1]), sl)
            return carry

        lax.fori_loop(0, 4, body, 0)

    def part_of(slot, sl, j):
        return jnp.dot(u_buf[sl, piece(j)], w_buf[slot, piece(j), :], preferred_element_type=F32)

    def project(slots):
        over(slots, lambda n, slot, sl: finish(jnp.dot(u_buf[sl, :], w_buf[slot], preferred_element_type=F32), slot, sl))

    def project_piece(slots, j):
        def fn(n, slot, sl):
            both = part_of(slot, sl, j) + part_of(slot, sl, j + few)
            if j > 0:
                both = acc[n, sl, :] + both
            if j < few - 1:
                acc[n, sl, :] = both
            else:
                finish(both, slot, sl)

        over(slots, fn)

    stores = []

    def store(slot, i):
        cp = pltpu.make_async_copy(w_buf.at[slot], all_ref.at[slot], out_sem.at[i])
        cp.start()
        stores.append(cp)

    for c in loads:
        c.wait()
    norm_rows = 64
    gain = gain_buf[...].astype(F32).reshape(1, dim)

    def norm(i, carry):
        sl = pl.ds(pl.multiple_of(i * norm_rows, norm_rows), norm_rows)
        x = u_buf[sl, :].astype(F32)
        mean_sq = jnp.sum(x * x, axis=-1, keepdims=True) * (1.0 / dim)
        u_buf[sl, :] = (x * lax.rsqrt(mean_sq + NORM_EPS) * gain).astype(BF16)
        return carry

    lax.fori_loop(0, seq // norm_rows, norm, 0)
    sent[own_mate].wait_recv()
    store(here, 0)
    store(mate, 1)
    project((here, mate))
    ls, rs, fs = to_left, to_right, 2 * far + core
    for j in range(few):
        sent[j].wait_recv()
        sent[on_right + j] = send(on_right + j, w_buf.at[ls, piece(j), :], ls, piece(j), to_right)
        sent[own_left + few + j].wait_recv()
        sent[on_left + j] = send(on_left + j, w_buf.at[rs, piece(few + j), :], rs, piece(few + j), to_left)
    sent[sides] = send(sides, w_buf.at[ls, A, :], ls, A, mate)
    sent[sides + 1] = send(sides + 1, w_buf.at[rs, B, :], rs, B, mate)
    for j in range(few):
        sent[few + j].wait_recv()
        sent[own_left + j].wait_recv()
    sent[sides + 2] = send(sides + 2, w_buf.at[ls, B, :], ls, B, mate)
    sent[sides + 3] = send(sides + 3, w_buf.at[rs, A, :], rs, A, mate)
    store(ls, 2)
    store(rs, 3)
    project((ls, rs))
    for i in range(4):
        sent[sides + i].wait_recv()
    store(2 * left + other, 4)
    store(2 * right + other, 5)
    project((2 * left + other, 2 * right + other))
    last = (fs, 2 * far + other)
    for j in range(few):
        a, b = ends + 2 * j, ends + 2 * j + 1
        sent[on_right + j].wait_recv()
        sent[a] = send(a, w_buf.at[fs, piece(j), :], fs, piece(j), mate)
        sent[on_left + j].wait_recv()
        sent[b] = send(b, w_buf.at[fs, piece(few + j), :], fs, piece(few + j), mate)
        sent[a].wait_recv()
        sent[b].wait_recv()
        if j == few - 1:
            store(last[0], 6)
            store(last[1], 7)
        project_piece(last, j)
    for cp in sent.values():
        cp.wait_send()
    for cp in stores:
        cp.wait()


def gather_qkv_call(n, x, gain, w, cos, sin):
    seq, dim = x.shape
    packed = w.shape[1]
    hd = packed // 3
    act = jax.ShapeDtypeStruct((n, seq, hd), BF16)
    any_spec = pl.BlockSpec(memory_space=pl.ANY)
    vmem = pl.BlockSpec(memory_space=pltpu.VMEM)
    return pl.pallas_call(
        functools.partial(gather_qkv_kernel, n // 2),
        in_specs=[any_spec] * 5,
        out_specs=[vmem, vmem, vmem, any_spec],
        out_shape=[act, act, act, jax.ShapeDtypeStruct((n, dim, packed), BF16)],
        scratch_shapes=[
            pltpu.VMEM((seq, dim), BF16),
            pltpu.VMEM((n, dim, packed), BF16),
            pltpu.VMEM((dim,), BF16),
            pltpu.VMEM((seq, hd // 2), F32),
            pltpu.VMEM((seq, hd // 2), F32),
            pltpu.VMEM((2, seq, packed), F32),
            pltpu.SemaphoreType.DMA((5,)),
            pltpu.SemaphoreType.DMA((n,)),
            pltpu.SemaphoreType.DMA((4 * PIECES + 5,)),
            pltpu.SemaphoreType.DMA((4 * PIECES + 5,)),
        ],
        compiler_params=pltpu.CompilerParams(collective_id=3, has_side_effects=True, vmem_limit_bytes=62 << 20),
        cost_estimate=pl.CostEstimate(flops=120_000_000_000, bytes_accessed=4 * dim * n * packed, transcendentals=0),
        name="gather_qkv",
    )(x, gain, w, cos, sin)


def unpack_kernel(w_ref, wq_ref, wk_ref, wv_ref):
    hd = w_ref.shape[2] // 3
    for i in range(2):
        cols = slice(i * hd, (i + 1) * hd)
        wq_ref[:, cols] = w_ref[i, :, 0:hd]
        wk_ref[:, cols] = w_ref[i, :, hd:2 * hd]
        wv_ref[:, cols] = w_ref[i, :, 2 * hd:3 * hd]


def unpack_call(wg):
    heads, dim, packed = wg.shape
    hd = packed // 3
    block = dim // 2
    wout = jax.ShapeDtypeStruct((dim, heads * hd), BF16)
    w_spec = pl.BlockSpec((block, 2 * hd), lambda h, r: (r, h))
    return pl.pallas_call(
        unpack_kernel,
        grid=(heads // 2, dim // block),
        in_specs=[pl.BlockSpec((2, block, packed), lambda h, r: (h, r, 0))],
        out_specs=[w_spec, w_spec, w_spec],
        out_shape=[wout, wout, wout],
        compiler_params=pltpu.CompilerParams(vmem_limit_bytes=62 << 20),
        cost_estimate=pl.CostEstimate(flops=dim * heads * packed, bytes_accessed=4 * dim * heads * packed, transcendentals=0),
        name="unpack",
    )(wg)


def gate_up_kernel(u_ref, w_ref, m_ref, wg_ref, wu_ref):
    ff = wg_ref.shape[1]
    wg_ref[0] = w_ref[0, 0:ff, :]
    wu_ref[0] = w_ref[0, ff:2 * ff, :]
    seq = u_ref.shape[0]
    tile = 1024

    def part(j, carry):
        sl = pl.ds(pl.multiple_of(j * tile, tile), tile)
        both = lax.dot_general(w_ref[0], u_ref[sl, :], (((1,), (1,)), ((), ())), preferred_element_type=F32)
        gate = both[0:ff].astype(BF16).astype(F32)
        up = both[ff:2 * ff].astype(BF16).astype(F32)
        m_ref[0, :, sl] = (gate * jax.nn.sigmoid(gate) * up).astype(BF16)
        return carry

    lax.fori_loop(0, seq // tile, part, 0)


def gate_up_call(u, wg):
    seq, dim = u.shape
    blocks, rows, _ = wg.shape
    ff = rows // 2
    wout = jax.ShapeDtypeStruct((blocks, ff, dim), BF16)
    wspec = pl.BlockSpec((1, ff, dim), lambda h: (h, 0, 0))
    return pl.pallas_call(
        gate_up_kernel,
        grid=(blocks,),
        in_specs=[
            pl.BlockSpec((seq, dim), lambda h: (0, 0), pipeline_mode=pl.Buffered(1)),
            pl.BlockSpec((1, rows, dim), lambda h: (h, 0, 0)),
        ],
        out_specs=[pl.BlockSpec((1, ff, seq), lambda h: (h, 0, 0)), wspec, wspec],
        out_shape=[jax.ShapeDtypeStruct((blocks, ff, seq), BF16), wout, wout],
        compiler_params=pltpu.CompilerParams(vmem_limit_bytes=60 << 20),
        cost_estimate=pl.CostEstimate(flops=2 * seq * dim * blocks * rows, bytes_accessed=4 * dim * blocks * rows, transcendentals=seq * ff * blocks),
        name="gate_up",
    )(u, wg)


CHUNKS = 2
COPIES = 12


def sum_kernel(n, transposed, col0, *refs):
    if transposed:
        a_ref, w_ref, res_ref, out_ref, *scratch = refs
    else:
        len_ref, q_ref, k_ref, v_ref, gain_ref, w_ref, res_ref, out_ref, norm_ref, norm_buf, norm_sem, *scratch = refs
    a_buf, w_buf, res_buf, part, own, first, second, gath, in_sem, out_sem, send_sem, recv_sem = scratch
    me = lax.axis_index("tpa")
    right, left, far = lax.rem(me + 1, n), lax.rem(me + n - 1, n), lax.rem(me + 2, n)
    order = (far, right, left, me)
    shard, width = own.shape
    half = width // 2
    rows = shard // CHUNKS
    tile = w_buf.shape[2]
    tiles = w_buf.shape[0]

    loads = []
    if transposed:
        for s in range(n):
            span = pl.ds(pl.multiple_of(order[s] * shard, shard), shard)
            loads.append(pltpu.make_async_copy(a_ref.at[:, span], a_buf.at[s], in_sem.at[s]))

    def wload(t):
        return pltpu.make_async_copy(w_ref.at[:, pl.ds(pl.multiple_of(t * tile, tile), tile)], w_buf.at[t], in_sem.at[n + t])

    mine = pl.ds(pl.multiple_of(me * shard, shard), shard)
    res_load = pltpu.make_async_copy(res_ref.at[mine, col0:col0 + width], res_buf, in_sem.at[n + tiles])
    for c in loads[:1] + [wload(t) for t in range(tiles)] + loads[1:] + [res_load]:
        c.start()

    barrier = pltpu.get_barrier_semaphore()
    for peer in (left, right):
        pl.semaphore_signal(barrier, inc=1, device_id={"tpa": peer}, device_id_type=MESH)
    pl.semaphore_wait(barrier, 2)

    A, B = slice(0, half), slice(half, width)

    def span_of(c):
        return slice(c * rows, (c + 1) * rows)

    def send(c, i, src, dst, peer):
        cp = pltpu.make_async_remote_copy(src_ref=src, dst_ref=dst, send_sem=send_sem.at[c, i], recv_sem=recv_sem.at[c, i], device_id={"tpa": peer}, device_id_type=MESH)
        cp.start()
        return cp

    dims = (((0,), (0,)), ((), ())) if transposed else (((1,), (0,)), ((), ()))

    def ready(s, owner):
        heads, _, hd = k_ref.shape
        base = pl.multiple_of(owner * shard, shard)
        length = len_ref[0]

        def head(h, carry):
            q = q_ref[h, pl.ds(base, shard), :]
            sc = lax.dot_general(q, k_ref[h], (((1,), (1,)), ((), ())), preferred_element_type=F32) * hd ** -0.5
            row = base + lax.broadcasted_iota(jnp.int32, sc.shape, 0)
            col = lax.broadcasted_iota(jnp.int32, sc.shape, 1)
            sc = jnp.where((col <= row) & (col < length), sc, MASK_VALUE)
            e = jnp.exp(sc - jnp.max(sc, axis=-1, keepdims=True))
            prob = (e * (1.0 / jnp.sum(e, axis=-1, keepdims=True))).astype(BF16)
            out = jnp.dot(prob, v_ref[h], preferred_element_type=F32).astype(BF16)
            a_buf[s, :, pl.ds(pl.multiple_of(h * hd, hd), hd)] = out
            return carry

        lax.fori_loop(0, heads, head, 0)

    def product(s, t):
        return lax.dot_general(a_buf[s], w_buf[t], dims, preferred_element_type=F32)

    def tile_loop(lo, hi, fn):
        def body(t, carry):
            fn(t, pl.ds(pl.multiple_of(t * tile, tile), tile))
            return carry

        lax.fori_loop(lo, hi, body, 0)

    sent = {}
    mid, quarter, wide = tiles // 2, tiles // 4, width // 4

    def far_copy(side, c, cols, start, peer):
        return pltpu.make_async_remote_copy(src_ref=part.at[0, :, cols], dst_ref=first.at[side, :, pl.ds(start, wide)], send_sem=send_sem.at[c, side], recv_sem=recv_sem.at[c, side], device_id={"tpa": peer}, device_id_type=MESH)

    if transposed:
        loads[0].wait()
    else:
        ready(0, far)

    def far_quarter(i, carry):
        side, c = lax.rem(i, 2), i // 2
        number = 2 * side + c

        def fn(t, cols):
            wload(t).wait()
            part[0, :, cols] = product(0, t).astype(BF16)

        tile_loop(number * quarter, (number + 1) * quarter, fn)
        cols = pl.ds(pl.multiple_of(number * wide, wide), wide)
        far_copy(side, c, cols, pl.multiple_of(c * wide, wide), jnp.where(side == 0, right, left)).start()
        return carry

    lax.fori_loop(0, 4, far_quarter, 0)
    for c in range(2):
        for side in range(2):
            number = 2 * side + c
            sent[c, side] = far_copy(side, c, slice(number * wide, (number + 1) * wide), c * wide, (right, left)[side])

    if transposed:
        loads[1].wait()
        loads[2].wait()
    else:
        def beside(s, carry):
            ready(s, jnp.where(s == 1, right, left))
            return carry

        lax.fori_loop(1, 3, beside, 0)

    def beside_tiles(i, carry):
        turn, job = i // tiles, lax.rem(i, tiles)
        s = 1 + job // mid
        t = lax.rem(job, mid) + mid * lax.rem(s + turn, 2)
        part[s, :, pl.ds(pl.multiple_of(t * tile, tile), tile)] = product(s, t).astype(BF16)

        @pl.when(i == mid - 1)
        def _():
            direct(2)

        @pl.when(i == tiles - 1)
        def _():
            direct(3)

        return carry

    def direct_copy(c, i):
        r = span_of(c)
        src, dst, peer = (part.at[1, r, B], second.at[0, r, B], right) if i == 2 else (part.at[2, r, A], second.at[1, r, A], left)
        return pltpu.make_async_remote_copy(src_ref=src, dst_ref=dst, send_sem=send_sem.at[c, i], recv_sem=recv_sem.at[c, i], device_id={"tpa": peer}, device_id_type=MESH)

    def direct(i):
        for c in range(CHUNKS):
            direct_copy(c, i).start()

    lax.fori_loop(0, 2 * tiles, beside_tiles, 0)
    for c in range(CHUNKS):
        for i in (2, 3):
            sent[c, i] = direct_copy(c, i)
    if transposed:
        loads[3].wait()
    else:
        ready(3, me)
    res_load.wait()

    def mine_too(t, cols):
        own[:, cols] = res_buf[:, cols].astype(F32) + product(3, t)

    tile_loop(0, tiles, mine_too)

    for c in range(CHUNKS):
        r = span_of(c)
        if c == 0:
            sent[0, 0].wait_recv()
            sent[1, 0].wait_recv()
        part[1, r, A] = (part[1, r, A].astype(F32) + first[0, r, :].astype(F32)).astype(BF16)
        sent[c, 4] = send(c, 4, part.at[1, r, A], second.at[0, r, A], right)
        if c == 0:
            sent[0, 1].wait_recv()
            sent[1, 1].wait_recv()
        part[2, r, B] = (part[2, r, B].astype(F32) + first[1, r, :].astype(F32)).astype(BF16)
        sent[c, 5] = send(c, 5, part.at[2, r, B], second.at[1, r, B], left)

    stores = []

    def normed(c, slot, owner):
        if transposed:
            return
        gain = gain_ref[...].astype(F32).reshape(1, width)
        step = 16

        def body(i, carry):
            sl = pl.ds(pl.multiple_of(c * rows + i * step, step), step)
            x = gath[slot, sl, :].astype(F32)
            mean_sq = jnp.sum(x * x, axis=-1, keepdims=True) * (1.0 / width)
            norm_buf[slot, sl, :] = (x * lax.rsqrt(mean_sq + NORM_EPS) * gain).astype(BF16)
            return carry

        lax.fori_loop(0, rows // step, body, 0)
        dst = norm_ref.at[pl.ds(pl.multiple_of(owner * shard + c * rows, rows), rows), :]
        cp = pltpu.make_async_copy(norm_buf.at[slot, span_of(c), :], dst, norm_sem.at[c, slot])
        cp.start()
        stores.append(cp)

    def store(c, slot, owner, i, cols):
        r = span_of(c)
        dst = out_ref.at[pl.ds(pl.multiple_of(owner * shard + c * rows, rows), rows), cols]
        cp = pltpu.make_async_copy(gath.at[slot, r, cols], dst, out_sem.at[c, i])
        cp.start()
        stores.append(cp)

    for c in range(CHUNKS):
        r = span_of(c)
        for i in (2, 4, 3, 5):
            sent[c, i].wait_recv()
        total = own[r, :] + second[0, r, :].astype(F32) + second[1, r, :].astype(F32)
        gath[0, r, :] = total.astype(BF16)
        sent[c, 6] = send(c, 6, gath.at[0, r, A], gath.at[1, r, A], right)
        sent[c, 7] = send(c, 7, gath.at[0, r, B], gath.at[2, r, B], left)
        sent[c, 8] = send(c, 8, gath.at[0, r, B], gath.at[1, r, B], right)
        sent[c, 9] = send(c, 9, gath.at[0, r, A], gath.at[2, r, A], left)
        store(c, 0, me, 0, slice(0, width))
    for c in range(CHUNKS):
        normed(c, 0, me)
    for c in range(CHUNKS):
        r = span_of(c)
        sent[c, 6].wait_recv()
        sent[c, 10] = send(c, 10, gath.at[1, r, A], gath.at[3, r, A], right)
        sent[c, 7].wait_recv()
        sent[c, 11] = send(c, 11, gath.at[2, r, B], gath.at[3, r, B], left)
        store(c, 1, left, 1, A)
        store(c, 2, right, 2, B)
    for c in range(CHUNKS):
        sent[c, 8].wait_recv()
        store(c, 1, left, 3, B)
        normed(c, 1, left)
        sent[c, 9].wait_recv()
        store(c, 2, right, 4, A)
        normed(c, 2, right)
    for c in range(CHUNKS):
        sent[c, 10].wait_recv()
        store(c, 3, far, 5, A)
        sent[c, 11].wait_recv()
        store(c, 3, far, 6, B)
        normed(c, 3, far)
    for cp in sent.values():
        cp.wait_send()
    for cp in stores:
        cp.wait()


def sum_call(n, a, w, res, col0, cid, transposed):
    depth, width = w.shape
    seq = res.shape[0]
    shard = seq // n
    tile = 512
    tiles = width // tile
    assert CHUNKS == 2 and tiles % 4 == 0
    any_spec = pl.BlockSpec(memory_space=pl.ANY)
    a_shape = (n, depth, shard) if transposed else (n, shard, depth)
    vmem = pl.BlockSpec(memory_space=pltpu.VMEM)
    head_specs = [any_spec] if transposed else [pl.BlockSpec(memory_space=pltpu.SMEM), vmem, vmem, vmem, vmem]
    out = jax.ShapeDtypeStruct((seq, width), BF16)
    norm_scratch = [] if transposed else [pltpu.VMEM((4, shard, width), BF16), pltpu.SemaphoreType.DMA((CHUNKS, 4))]
    return pl.pallas_call(
        functools.partial(sum_kernel, n, transposed, col0),
        in_specs=head_specs + [any_spec] * 2,
        out_specs=any_spec if transposed else [any_spec] * 2,
        out_shape=out if transposed else [out] * 2,
        scratch_shapes=norm_scratch + [
            pltpu.VMEM(a_shape, BF16),
            pltpu.VMEM((tiles, depth, tile), BF16),
            pltpu.VMEM((shard, width), BF16),
            pltpu.VMEM((3, shard, width), BF16),
            pltpu.VMEM((shard, width), F32),
            pltpu.VMEM((2, shard, width // 2), BF16),
            pltpu.VMEM((2, shard, width), BF16),
            pltpu.VMEM((4, shard, width), BF16),
            pltpu.SemaphoreType.DMA((n + tiles + 1,)),
            pltpu.SemaphoreType.DMA((CHUNKS, 7)),
            pltpu.SemaphoreType.DMA((CHUNKS, COPIES)),
            pltpu.SemaphoreType.DMA((CHUNKS, COPIES)),
        ],
        compiler_params=pltpu.CompilerParams(collective_id=cid, has_side_effects=True, vmem_limit_bytes=62 << 20),
        cost_estimate=pl.CostEstimate(flops=2 * seq * depth * width + 130_000_000_000, bytes_accessed=2 * depth * width, transcendentals=0),
    )(*a, w, res)


def copy_kernel(src_ref, dst_ref):
    dst_ref[...] = src_ref[...]


def copy_call(w):
    rows, width = w.shape
    block = rows // 8
    spec = pl.BlockSpec((block, width), lambda i: (i, 0))
    return pl.pallas_call(
        copy_kernel,
        grid=(rows // block,),
        in_specs=[spec],
        out_specs=spec,
        out_shape=jax.ShapeDtypeStruct((rows, width), w.dtype),
        compiler_params=pltpu.CompilerParams(vmem_limit_bytes=62 << 20),
        cost_estimate=pl.CostEstimate(flops=rows * width, bytes_accessed=4 * rows * width, transcendentals=0),
    )(w)


def finish_kernel(ya_ref, yb_ref, da_ref, db_ref, y_ref, d_ref):
    half = ya_ref.shape[1]
    y_ref[:, :half] = ya_ref[...]
    y_ref[:, half:] = yb_ref[...]
    d_ref[:, :half] = da_ref[...]
    d_ref[:, half:] = db_ref[...]


def finish_call(y_a, y_b, d_a, d_b):
    steps = 8
    seq, half = y_a.shape
    ff = d_a.shape[0]

    def spec(rows, width):
        return pl.BlockSpec((rows // steps, width), lambda i: (i, 0))

    return pl.pallas_call(
        finish_kernel,
        grid=(steps,),
        in_specs=[spec(seq, half), spec(seq, half), spec(ff, half), spec(ff, half)],
        out_specs=[spec(seq, 2 * half), spec(ff, 2 * half)],
        out_shape=[jax.ShapeDtypeStruct((seq, 2 * half), BF16), jax.ShapeDtypeStruct((ff, 2 * half), BF16)],
        compiler_params=pltpu.CompilerParams(vmem_limit_bytes=62 << 20),
        cost_estimate=pl.CostEstimate(flops=ff * half, bytes_accessed=8 * (seq + ff) * half, transcendentals=0),
        name="finish",
    )(y_a, y_b, d_a, d_b)


def solution(mesh):
    n_tpa = mesh.shape['tpa']
    assert n_tpa == 4

    def gather(w, tiled):
        return lax.all_gather(w, 'tpb', axis=0, tiled=tiled)

    def layer(x_loc, len_loc, k_buf, v_buf, w_qkv, w_o, w_gate_up, w_down, g_attn, g_mlp):
        seq, dim = x_loc.shape[1:]
        _, hd = k_buf.shape[2:]
        half = dim // 2
        x = x_loc[0]
        cos, sin = rope_tables(seq, hd)
        o_g = gather(w_o, True)
        q, k, v, qkv_g = gather_qkv_call(mesh.shape['tpb'], x, g_attn, w_qkv, cos, sin)
        gu_in, d_in, q = lax.optimization_barrier((w_gate_up.T, w_down, q))
        gu_g = gather(gu_in, False)
        down_a = gather(d_in[:, :half], True)
        down_b = gather(d_in[:, half:], True)
        hidden, u2 = sum_call(n_tpa, (len_loc, q, k, v, g_mlp), o_g, x, 0, 0, False)

        hidden, u2, k, v, o_g, qkv_g = lax.optimization_barrier((hidden, u2, k, v, o_g, qkv_g))
        valid = (jnp.arange(seq) < len_loc[0])[:, None, None]
        k_cache = jnp.where(valid, k.transpose(1, 0, 2), k_buf[0])[None]
        v_cache = jnp.where(valid, v.transpose(1, 0, 2), v_buf[0])[None]
        o_out = copy_call(o_g)
        w_q, w_k, w_v = unpack_call(qkv_g)
        u2, k_cache, v_cache, o_out, w_q, w_k, w_v = lax.optimization_barrier((u2, k_cache, v_cache, o_out, w_q, w_k, w_v))
        m_t, gate_t, up_t = gate_up_call(u2, gu_g)
        ff = m_t.shape[0] * m_t.shape[1]
        m_t = m_t.reshape(ff, seq)
        y_a = sum_call(n_tpa, (m_t,), down_a, hidden, 0, 1, True)
        y_b = sum_call(n_tpa, (m_t,), down_b, hidden, half, 2, True)
        y, down = finish_call(y_a, y_b, down_a, down_b)
        return (y[None], k_cache, v_cache, w_q, w_k, w_v, o_out, gate_t.reshape(ff, dim).T, up_t.reshape(ff, dim).T, down)

    batch_spec = P(('part', 'tpb'), None, None)
    len_spec = P(('part', 'tpb'))
    cache_spec = P(('part', 'tpb'), None, 'tpa', None)
    train_cols = P('part', ('tpa', 'tpb'))
    train_rows = P(('part', 'tpa', 'tpb'), None)
    gain_spec = P('part')
    gen_cols = P('part', 'tpa')
    gen_rows = P(('part', 'tpa'), None)
    return jax.shard_map(layer, mesh=mesh, in_specs=(batch_spec, len_spec, cache_spec, cache_spec, train_cols, train_rows, train_cols, train_rows, gain_spec, gain_spec), out_specs=(batch_spec, cache_spec, cache_spec, gen_cols, gen_cols, gen_cols, gen_rows, gen_cols, gen_cols, gen_rows), check_vma=False)
```
